32 devices in a mesh: up: 8 (over z, core), down: 4 (over y, x).
Axes of the slice: x: 2, y: 2, z: 4, core: 2. Of those that a mesh axis runs over, the one named last changes fastest.
Arguments:
- deltas: bfloat16 [256, 4096], P('down', 'up'), may hold values from -6 to 6
- gradients: bfloat16 [256, 4096], P('up', 'down'), may hold values from -0.375 to 0.375
- up_blocks: int32 [8, 16], P(None, 'up'), may hold values from 0 to 3, as said below
- down_blocks: int32 [16], P('down'), may hold values from 0 to 7, as said below
- decoder: bfloat16 [4096, 4608], P('up', 'down'), may hold values from -0.09375 to 0.09375
- encoder: bfloat16 [4608, 4096], P('up', 'down'), may hold values from -6 to 6
Outputs:
- edge_scores: float32 [4096, 4096], P('up', 'down')
The draws below stay inside these ranges and needn't reach their ends.
Inputs may be any that keep to these rules, and one draw needn't show every extreme that they name: `up_blocks`: for each window and each index i of up, the 2 entries in columns i * 2 to (i + 1) * 2 - 1 are distinct. `down_blocks`: for each index j of down, the 4 entries j * 4 to (j + 1) * 4 - 1 are distinct.
All inputs are finite; a program needn't handle non-finite values.
Results may differ from the reference program's by a relative error of at most 0.0003.
Values may be sent and summed in bfloat16 or wider, within the bound.
A program may use at most 64 MiB of HBM per device.

```python
import jax
import jax.numpy as jnp
from jax import lax

D = 4608
VF_DEV = 1024
BLOCK = 128
UACT = 2
DACT = 4
WIN = 32
TOKENS = 256
WINDOWS = 8
UB_DEV = 4
VB_DEV = 8
UF = 4096
VF = 4096
N_UP = 8
N_DOWN = 4


def draw_up_blocks(key, part):
    ranked = jax.random.randint(key, (WINDOWS, N_UP, UB_DEV), 0, 1 << 20, dtype=jnp.int32)
    ranked = ranked * UB_DEV + jnp.arange(UB_DEV, dtype=jnp.int32)
    ordering = jnp.argsort(ranked, axis=-1, stable=True)
    return ordering[:, :, :UACT].reshape(WINDOWS, N_UP * UACT).astype(jnp.int32)


def draw_down_blocks(key, part):
    ranked = jax.random.randint(jax.random.fold_in(key, 7), (N_DOWN, VB_DEV), 0, 1 << 20, dtype=jnp.int32)
    ranked = ranked * VB_DEV + jnp.arange(VB_DEV, dtype=jnp.int32)
    ordering = jnp.argsort(ranked, axis=-1, stable=True)
    return ordering[:, :DACT].reshape(N_DOWN * DACT).astype(jnp.int32)


def level_of(key, shape, cuts, low, high):
    gain, own = 1.0, jax.random.fold_in(key, 6)
    for position, blocks in cuts:
        heights = jnp.exp(jax.random.uniform(jax.random.fold_in(own, position), (blocks,), jnp.float32, low / len(cuts), high / len(cuts)))
        gain = gain * jnp.repeat(heights, shape[position] // blocks).reshape([-1 if axis == position else 1 for axis in range(len(shape))])
    return gain


def normal_values(key, dims, scale, bound, split=(), kind=jnp.bfloat16):
    gain = level_of(key, dims, split, -0.22, 0.18) if split else 1.0
    drawn = jax.random.normal(key, dims, jnp.float32) * scale * gain
    return jnp.minimum(jnp.maximum(drawn, -bound), bound).astype(kind)


def setup_inputs(seed: int = 0) -> dict:
    key_of = jax.random.split(jax.random.key(seed), 7)
    return {
        "deltas": normal_values(key_of[0], (TOKENS, UF), 1.0, 6.0, ((0, 4), (1, 8))),
        "gradients": normal_values(key_of[1], (TOKENS, VF), TOKENS ** -0.5, 0.375, ((0, 8), (1, 4))),
        "up_blocks": draw_up_blocks(jax.random.fold_in(key_of[6], 71), 0),
        "down_blocks": draw_down_blocks(jax.random.fold_in(key_of[6], 71), 0),
        "decoder": normal_values(key_of[4], (UF, D), D ** -0.5, 0.09375, ((0, 8), (1, 4))),
        "encoder": normal_values(key_of[5], (D, VF), 1.0, 6.0, ((0, 8), (1, 4))),
    }


def reference(deltas, gradients, up_blocks, down_blocks, decoder, encoder):
    owners = (jnp.arange(N_UP * UACT, dtype=jnp.int32) // UACT) * UB_DEV
    global_ids = up_blocks + owners[None, :]
    every_block = jnp.arange(N_UP * UB_DEV, dtype=jnp.int32)
    block_on = jnp.any(global_ids[:, :, None] == every_block[None, None, :], axis=1)
    masked = deltas.reshape(WINDOWS, WIN, N_UP * UB_DEV, BLOCK) * block_on[:, None, :, None].astype(deltas.dtype)
    masked = masked.reshape(TOKENS, UF)

    def shard_scores(shard_index):
        enc_cols = lax.dynamic_slice_in_dim(encoder, shard_index * VF_DEV, VF_DEV, 1).reshape(D, VB_DEV, BLOCK)
        grad_cols = lax.dynamic_slice_in_dim(gradients, shard_index * VF_DEV, VF_DEV, 1).reshape(TOKENS, VB_DEV, BLOCK)
        chosen = lax.dynamic_slice_in_dim(down_blocks, shard_index * DACT, DACT, 0)
        enc_used = jnp.take(enc_cols, chosen, axis=1).reshape(D, DACT * BLOCK)
        grad_used = jnp.take(grad_cols, chosen, axis=1).reshape(TOKENS, DACT * BLOCK)
        virtual = jnp.dot(decoder, enc_used, preferred_element_type=jnp.float32)
        product = lax.dot_general(masked, grad_used, (((0,), (0,)), ((), ())), preferred_element_type=jnp.float32)
        scored = (product * virtual).reshape(UF, DACT, BLOCK)
        filled = jnp.zeros((UF, VB_DEV, BLOCK), jnp.float32).at[:, chosen, :].set(scored)
        return filled.reshape(UF, VF_DEV)

    stacked = lax.map(shard_scores, jnp.arange(N_DOWN, dtype=jnp.int32))
    return jnp.transpose(stacked, (1, 0, 2)).reshape(UF, VF)
```

```python
import functools

import jax
import jax.numpy as jnp
from jax import lax
from jax.experimental import pallas as pl
from jax.experimental.pallas import tpu as pltpu
from jax.sharding import PartitionSpec as P

BLOCK = 128
MESH = pl.DeviceIdType.MESH
F32 = jnp.float32


def flag(number, block, kind):
    return jnp.where(jnp.full((1, BLOCK), number, jnp.int32) == block, 1.0, 0.0).astype(kind)


def pick(ref, rows, number, blocks):
    total = None
    for b in range(blocks):
        term = ref[rows, b * BLOCK:(b + 1) * BLOCK] * flag(number, b, ref.dtype)
        total = term if total is None else total + term
    return total


def gather_scores(
    n_up, n_down, upb, downb, deltas, grads, dec, enc, out,
    dec_all, enc_raw, enc_all, del_raw, del_all, grad_raw, grad_all, masked, acc, prod,
    load_sem, dec_send, dec_recv, del_send, del_recv, enc_send, enc_recv,
    grad_send, grad_recv, pair_send, pair_recv, pg_send, pg_recv,
):
    levels = n_up // 2
    rows, depth = dec.shape
    height = enc.shape[0]
    half = height // 2
    chunk = rows // 4
    toks = grads.shape[0]
    wins = del_all.shape[1]
    win = del_all.shape[2]
    uact = upb.shape[1]
    dact = downb.shape[0]
    up, down = lax.axis_index("up"), lax.axis_index("down")
    z, core = up // 2, up % 2
    place = lambda d: 2 * (d // 2) + (d + d // 2) % 2
    pos = place(down)
    right, left = place((pos + 1) % 4), place((pos + 3) % 4)
    diag = place((pos + 2) % 4)
    ring_to = ((up, right), (up, left))
    ring_from = (left, right)
    step_of = (1, -1)

    loads = [
        pltpu.make_async_copy(dec, dec_all.at[down], load_sem.at[0]),
        pltpu.make_async_copy(enc, enc_raw, load_sem.at[1]),
        pltpu.make_async_copy(deltas, del_raw, load_sem.at[2]),
        pltpu.make_async_copy(grads, grad_raw, load_sem.at[3]),
    ]
    for copy in loads:
        copy.start()

    barrier = pltpu.get_barrier_semaphore()
    can_go = (z < levels - 1, z > 0)
    for dev in (*ring_to, (2 * z + 1 - core, down)):
        pl.semaphore_signal(barrier, inc=1, device_id=dev, device_id_type=MESH)
    for r in range(2):
        @pl.when(can_go[r])
        def _():
            pl.semaphore_signal(barrier, inc=1, device_id=(up + 2 * step_of[r], down), device_id_type=MESH)

    loads[2].wait()
    for w in range(wins):
        for s in range(uact):
            del_all[down, w, :, s * BLOCK:(s + 1) * BLOCK] = pick(
                del_raw, slice(w * win, (w + 1) * win), upb[down * wins + w, s], rows // BLOCK)
    loads[3].wait()
    loads[1].wait()
    for s in range(dact):
        grad_all[pl.ds(pl.multiple_of(up * toks, toks), toks), s * BLOCK:(s + 1) * BLOCK] = pick(
            grad_raw, slice(0, toks), downb[s], enc.shape[1] // BLOCK)
        enc_all[pl.ds(pl.multiple_of(up * height, 16), height), s * BLOCK:(s + 1) * BLOCK] = pick(
            enc_raw, slice(0, height), downb[s], enc.shape[1] // BLOCK)
    loads[0].wait()
    expected = 3 + jnp.where(z < levels - 1, 1, 0) + jnp.where(z > 0, 1, 0)
    pl.semaphore_wait(barrier, expected)

    orders = ((0, 1, 2, 3), (2, 3, 0, 1))

    def dec_copy(r, i, owner):
        piece = orders[r][i % 4]
        ref = dec_all.at[owner, pl.ds(piece * chunk, chunk)]
        return pltpu.make_async_remote_copy(
            ref, ref, dec_send.at[r, i], dec_recv.at[r, i], device_id=ring_to[r], device_id_type=MESH)

    def del_copy(r, i, owner):
        piece = (i + r) % 2
        ref = del_all.at[owner, piece]
        return pltpu.make_async_remote_copy(
            ref, ref, del_send.at[r, i], del_recv.at[r, i], device_id=ring_to[r], device_id_type=MESH)

    def enc_rows(level, h, c):
        return enc_all.at[pl.ds(pl.multiple_of((level * 2 + c) * height + h * half, 16), half)]

    def enc_copy(r, k, level):
        ref = enc_rows(level, (k - 1) % 2, core)
        return pltpu.make_async_remote_copy(
            ref, ref, enc_send.at[r, k - 1], enc_recv.at[r, k - 1],
            device_id=(up + 2 * step_of[r], down), device_id_type=MESH)

    def grad_rows(level, c):
        return grad_all.at[pl.ds(pl.multiple_of((level * 2 + c) * toks, toks), toks)]

    def grad_copy(r, j, level):
        ref = grad_rows(level, core)
        return pltpu.make_async_remote_copy(
            ref, ref, grad_send.at[r, j - 1], grad_recv.at[r, j - 1],
            device_id=(up + 2 * step_of[r], down), device_id_type=MESH)

    def pair_copy(level, h, c):
        ref = enc_rows(level, h, c)
        return pltpu.make_async_remote_copy(
            ref, ref, pair_send.at[level, h], pair_recv.at[level, h],
            device_id=(2 * z + 1 - core, down), device_id_type=MESH)

    def pair_grad(level, c):
        ref = grad_rows(level, c)
        return pltpu.make_async_remote_copy(
            ref, ref, pg_send.at[level], pg_recv.at[level],
            device_id=(2 * z + 1 - core, down), device_id_type=MESH)

    inside = lambda level: jnp.logical_and(level >= 0, level < levels)

    for r in range(2):
        del_copy(r, 0, down).start()
        del_copy(r, 1, down).start()

        @pl.when(can_go[r])
        def _():
            grad_copy(r, 1, z).start()
    for i in range(2):
        for r in range(2):
            dec_copy(r, i, down).start()

            @pl.when(can_go[r])
            def _():
                enc_copy(r, i + 1, z).start()
    for i in range(2, 4):
        for r in range(2):
            dec_copy(r, i, down).start()
    pair_grad(z, core).start()
    for h in range(2):
        pair_copy(z, h, core).start()

    def quarter(q):
        for m in range(2):
            for n in range(2):
                rs, cs = slice(m * rows // 2, (m + 1) * rows // 2), slice(n * acc.shape[1] // 2, (n + 1) * acc.shape[1] // 2)
                acc[rs, cs] += jnp.dot(
                    dec_all[q, rs, :], enc_all[pl.ds(pl.multiple_of(q * depth, 128), depth), cs],
                    preferred_element_type=F32)

    far = lambda q: jnp.maximum(q - z, z - q) >= levels - 1
    late = [jnp.where(jnp.logical_or(diag == q, far(q)), 1, 0) for q in range(levels)]
    early = sum(1 - x for x in late)
    rank = []
    for q in range(levels):
        before = sum(late[:q]) if q else 0
        rank.append(jnp.where(late[q] == 1, early + before, q - before))
    order = [sum(jnp.where(rank[q] == s, q, 0) for q in range(levels)) for s in range(levels)]

    acc[...] = jnp.zeros_like(acc)

    for k in range(1, 2 * (levels - 1) + 1):
        j, h = (k + 1) // 2, (k - 1) % 2
        for r in range(2):
            if k == 1:
                del_copy(r, 0, ring_from[r]).wait_recv()
                del_copy(r, 2, ring_from[r]).start()
            if k <= 2:
                dec_copy(r, k - 1, ring_from[r]).wait_recv()
                dec_copy(r, k + 3, ring_from[r]).start()
        for r in range(2):
            level = z - step_of[r] * j

            @pl.when(inside(level))
            def _():
                if h == 0:
                    grad_copy(r, j, level).wait_recv()
                    if j < levels - 1:
                        @pl.when(can_go[r])
                        def _():
                            grad_copy(r, j + 1, level).start()
                    pair_grad(level, core).start()
                enc_copy(r, k, level).wait_recv()
                if j < levels - 1:
                    @pl.when(can_go[r])
                    def _():
                        enc_copy(r, k + 2, level).start()
                pair_copy(level, h, core).start()
        if k == 2 * (levels - 2):
            for r in range(2):
                for i in range(2, 4):
                    dec_copy(r, i, ring_from[r]).wait_recv()
            for lv in range(levels):
                @pl.when(jnp.logical_not(far(lv)))
                def _():
                    for h2 in range(2):
                        pair_copy(lv, h2, 1 - core).wait_recv()

            @pl.loop(0, 2)
            def _(s):
                quarter(jnp.where(s == 0, order[0], order[1]))
        if k == 2 * (levels - 2) + 1:
            for r in range(2):
                del_copy(r, 1, ring_from[r]).wait_recv()
                del_copy(r, 2, diag).wait_recv()
            for lv in range(levels):
                pair_grad(lv, 1 - core).wait_recv()
            for d in range(n_down):
                for w in range(wins):
                    for b in range(rows // BLOCK):
                        value = jnp.zeros((win, BLOCK), masked.dtype)
                        for s in range(uact):
                            on = flag(upb[d * wins + w, s], b, masked.dtype)
                            value = value + del_all[d, w, :, s * BLOCK:(s + 1) * BLOCK] * on
                        t = (d * wins + w) * win
                        masked[t:t + win, b * BLOCK:(b + 1) * BLOCK] = value
            prod[...] = lax.dot_general(
                masked[...], grad_all[...], (((0,), (0,)), ((), ())), preferred_element_type=F32)

    for r in range(2):
        for i in range(4, 6):
            dec_copy(r, i, diag).wait_recv()
    for lv in range(levels):
        @pl.when(far(lv))
        def _():
            for h2 in range(2):
                pair_copy(lv, h2, 1 - core).wait_recv()

    @pl.loop(2, 4)
    def _(s):
        quarter(jnp.where(s == 2, order[2], order[3]))
    out[...] = acc[...] * prod[...]

    for r in range(2):
        for i in range(3):
            del_copy(r, i, down).wait_send()
        for i in range(6):
            dec_copy(r, i, down).wait_send()
        for k in range(1, 2 * (levels - 1) + 1):
            @pl.when(jnp.logical_and(can_go[r], inside(z - step_of[r] * ((k - 1) // 2))))
            def _():
                enc_copy(r, k, z).wait_send()
                if k % 2:
                    grad_copy(r, (k + 1) // 2, z).wait_send()
    for lv in range(levels):
        pair_grad(lv, core).wait_send()
        for h in range(2):
            pair_copy(lv, h, core).wait_send()


def spread(downb, scored, out):
    for c in range(out.shape[1] // BLOCK):
        slot, on = 0, 0
        for s in range(downb.shape[0]):
            hit = (downb[s] == c).astype(jnp.int32)
            slot, on = slot + s * hit, on + hit
        value = scored[:, pl.ds(pl.multiple_of(slot * BLOCK, BLOCK), BLOCK)]
        out[:, c * BLOCK:(c + 1) * BLOCK] = jnp.where(on > 0, value, 0.0)


def ring_local(n_up, n_down, win, deltas, gradients, up_blocks, down_blocks, decoder, encoder):
    rows, depth = decoder.shape
    height, cols = encoder.shape
    toks = gradients.shape[0]
    uact, dact = up_blocks.shape[1], down_blocks.shape[0]
    tokens = deltas.shape[0] * n_down
    wins = deltas.shape[0] // win
    used = dact * BLOCK
    levels = n_up // 2
    kind = decoder.dtype
    dma = pltpu.SemaphoreType.DMA
    smem, anywhere = pl.BlockSpec(memory_space=pltpu.SMEM), pl.BlockSpec(memory_space=pl.ANY)
    vmem = pl.BlockSpec(memory_space=pltpu.VMEM)
    hops = 2 * (levels - 1)
    scored = pl.pallas_call(
        functools.partial(gather_scores, n_up, n_down),
        out_shape=jax.ShapeDtypeStruct((rows, used), F32),
        in_specs=[smem, smem, anywhere, anywhere, anywhere, anywhere],
        out_specs=vmem,
        scratch_shapes=[
            pltpu.VMEM((n_down, rows, depth), kind),
            pltpu.VMEM((height, cols), kind),
            pltpu.VMEM((n_up * height, used), kind),
            pltpu.VMEM(deltas.shape, kind),
            pltpu.VMEM((n_down, wins, win, uact * BLOCK), kind),
            pltpu.VMEM((toks, cols), kind),
            pltpu.VMEM((n_up * toks, used), kind),
            pltpu.VMEM((tokens, rows), kind),
            pltpu.VMEM((rows, used), F32),
            pltpu.VMEM((rows, used), F32),
            dma((4,)),
            dma((2, 6)), dma((2, 6)),
            dma((2, 3)), dma((2, 3)),
            dma((2, hops)), dma((2, hops)),
            dma((2, levels - 1)), dma((2, levels - 1)),
            dma((levels, 2)), dma((levels, 2)),
            dma((levels,)), dma((levels,)),
        ],
        compiler_params=pltpu.CompilerParams(collective_id=0, has_side_effects=True),
        name="gather_scores",
    )(up_blocks, down_blocks, deltas, gradients, decoder, encoder)
    tile = rows // 4
    return pl.pallas_call(
        spread,
        grid=(rows // tile,),
        out_shape=jax.ShapeDtypeStruct((rows, cols), F32),
        in_specs=[smem, pl.BlockSpec((tile, used), lambda i: (i, 0))],
        out_specs=pl.BlockSpec((tile, cols), lambda i: (i, 0)),
        name="spread",
    )(down_blocks, scored)


def plain_local(deltas, gradients, up_blocks, down_blocks, decoder, encoder):
    token_deltas = lax.all_gather(deltas, "down", axis=0, tiled=True)
    token_grads = lax.all_gather(gradients, "up", axis=0, tiled=True)
    tokens, rows = token_deltas.shape
    windows, dact = up_blocks.shape[0], down_blocks.shape[0]
    row_blocks, col_blocks = rows // BLOCK, encoder.shape[1] // BLOCK
    local_ids = jnp.arange(row_blocks, dtype=jnp.int32)
    block_on = jnp.any(up_blocks[:, :, None] == local_ids[None, None, :], axis=1)
    masked = token_deltas.reshape(windows, tokens // windows, row_blocks, BLOCK) * block_on[
        :, None, :, None].astype(token_deltas.dtype)
    masked = masked.reshape(tokens, rows)
    dec_whole = lax.all_gather(decoder, "down", axis=1, tiled=True)
    height = encoder.shape[0]
    enc_used = jnp.take(encoder.reshape(height, col_blocks, BLOCK), down_blocks, axis=1).reshape(height, dact * BLOCK)
    virtual = jnp.dot(dec_whole, lax.all_gather(enc_used, "up", axis=0, tiled=True), preferred_element_type=F32)
    grad_used = jnp.take(token_grads.reshape(tokens, col_blocks, BLOCK), down_blocks, axis=1).reshape(tokens, dact * BLOCK)
    product = lax.dot_general(masked, grad_used, (((0,), (0,)), ((), ())), preferred_element_type=F32)
    scored = (product * virtual).reshape(rows, dact, BLOCK)
    filled = jnp.zeros((rows, col_blocks, BLOCK), F32).at[:, down_blocks, :].set(scored)
    return filled.reshape(rows, encoder.shape[1])


def solution(mesh):
    n_up, n_down = mesh.shape["up"], mesh.shape["down"]
    ringed = n_down == 4 and n_up == 2 * n_down

    def local(deltas, gradients, up_blocks, down_blocks, decoder, encoder):
        args = (deltas, gradients, up_blocks, down_blocks, decoder, encoder)
        tokens = deltas.shape[0] * n_down
        win = tokens // up_blocks.shape[0]
        if ringed and deltas.shape[0] == 2 * win:
            return ring_local(n_up, n_down, win, *args)
        return plain_local(*args)

    placed = (P("down", "up"), P("up", "down"), P(None, "up"), P("down"), P("up", "down"), P("up", "down"))
    return jax.shard_map(local, mesh=mesh, in_specs=placed, out_specs=P("up", "down"), check_vma=False)
```

```python
import functools

import jax
import jax.numpy as jnp
from jax import lax
from jax.experimental import pallas as pl
from jax.experimental.pallas import tpu as pltpu
from jax.sharding import PartitionSpec as P

BLOCK = 128
LARGE, SMALL = 24 << 20, 4 << 20
MESH = pl.DeviceIdType.MESH
F32 = jnp.float32


def flag(number, block, kind):
    return jnp.where(jnp.full((1, BLOCK), number, jnp.int32) == block, 1.0, 0.0).astype(kind)


def pick(ref, rows, number, blocks):
    total = None
    for b in range(blocks):
        term = ref[rows, b * BLOCK:(b + 1) * BLOCK] * flag(number, b, ref.dtype)
        total = term if total is None else total + term
    return total


def gather_scores(
    n_up, n_down, upb, downb, deltas, grads, dec, enc, out,
    dec_all, enc_raw, enc_all, del_raw, del_all, grad_raw, grad_all, masked, acc, prod, res,
    load_sem, dec_send, dec_recv, del_send, del_recv, enc_send, enc_recv,
    grad_send, grad_recv, pair_send, pair_recv, pg_send, pg_recv, out_sem,
):
    levels = n_up // 2
    rows, depth = dec.shape
    height = enc.shape[0]
    half = enc_all.shape[2]
    chunk = rows // 4
    toks = grads.shape[0]
    wins = del_all.shape[1]
    win = del_all.shape[2]
    uact = upb.shape[0]
    dact = downb.shape[0]
    up, down = lax.axis_index("up"), lax.axis_index("down")
    z, core = up // 2, up % 2
    place = lambda d: 2 * (d // 2) + (d + d // 2) % 2
    pos = place(down)
    right, left = place((pos + 1) % 4), place((pos + 3) % 4)
    diag = place((pos + 2) % 4)
    ring_to = ((up, right), (up, left))
    ring_from = (left, right)
    step_of = (1, -1)

    loads = [
        pltpu.make_async_copy(dec, dec_all.at[down], load_sem.at[0]),
        pltpu.make_async_copy(enc, enc_raw, load_sem.at[1]),
        pltpu.make_async_copy(deltas, del_raw, load_sem.at[2]),
        pltpu.make_async_copy(grads, grad_raw, load_sem.at[3]),
    ]
    for copy in loads:
        copy.start()

    barrier = pltpu.get_barrier_semaphore()
    can_go = (z < levels - 1, z > 0)
    for dev in (*ring_to, (2 * z + 1 - core, down)):
        pl.semaphore_signal(barrier, inc=1, device_id=dev, device_id_type=MESH)
    for r in range(2):
        @pl.when(can_go[r])
        def _():
            pl.semaphore_signal(barrier, inc=1, device_id=(up + 2 * step_of[r], down), device_id_type=MESH)

    loads[2].wait()
    for w in range(wins):
        for s in range(uact):
            del_all[down, w, :, s * BLOCK:(s + 1) * BLOCK] = pick(
                del_raw, slice(w * win, (w + 1) * win), upb[s, down * wins + w], rows // BLOCK)
    loads[3].wait()
    loads[1].wait()
    for s in range(dact):
        grad_all[pl.ds(pl.multiple_of(up * toks, toks), toks), s * BLOCK:(s + 1) * BLOCK] = pick(
            grad_raw, slice(0, toks), downb[s], enc.shape[1] // BLOCK)
        side, at = divmod(s * BLOCK, half)
        enc_all[side, pl.ds(pl.multiple_of(up * height, 16), height), at:at + BLOCK] = pick(
            enc_raw, slice(0, height), downb[s], enc.shape[1] // BLOCK)
    loads[0].wait()
    expected = 3 + jnp.where(z < levels - 1, 1, 0) + jnp.where(z > 0, 1, 0)
    pl.semaphore_wait(barrier, expected)

    orders = ((0, 2, 1, 3), (1, 3, 0, 2))

    def dec_copy(r, i, owner):
        piece = orders[r][i % 4]
        ref = dec_all.at[owner, pl.ds(piece * chunk, chunk)]
        return pltpu.make_async_remote_copy(
            ref, ref, dec_send.at[r, i], dec_recv.at[r, i], device_id=ring_to[r], device_id_type=MESH)

    def del_copy(r, i, owner):
        piece = (i + r) % 2
        ref = del_all.at[owner, piece]
        return pltpu.make_async_remote_copy(
            ref, ref, del_send.at[r, i], del_recv.at[r, i], device_id=ring_to[r], device_id_type=MESH)

    def enc_rows(level, h, c):
        return enc_all.at[h, pl.ds(pl.multiple_of((level * 2 + c) * height, 16), height)]

    def enc_copy(r, k, level):
        ref = enc_rows(level, (k - 1) % 2, core)
        return pltpu.make_async_remote_copy(
            ref, ref, enc_send.at[r, k - 1], enc_recv.at[r, k - 1],
            device_id=(up + 2 * step_of[r], down), device_id_type=MESH)

    def grad_rows(level, c):
        return grad_all.at[pl.ds(pl.multiple_of((level * 2 + c) * toks, toks), toks)]

    def grad_copy(r, j, level):
        ref = grad_rows(level, core)
        return pltpu.make_async_remote_copy(
            ref, ref, grad_send.at[r, j - 1], grad_recv.at[r, j - 1],
            device_id=(up + 2 * step_of[r], down), device_id_type=MESH)

    def pair_copy(level, h, c):
        ref = enc_rows(level, h, c)
        return pltpu.make_async_remote_copy(
            ref, ref, pair_send.at[level, h], pair_recv.at[level, h],
            device_id=(2 * z + 1 - core, down), device_id_type=MESH)

    def pair_grad(level, c):
        ref = grad_rows(level, c)
        return pltpu.make_async_remote_copy(
            ref, ref, pg_send.at[level], pg_recv.at[level],
            device_id=(2 * z + 1 - core, down), device_id_type=MESH)

    inside = lambda level: jnp.logical_and(level >= 0, level < levels)

    for r in range(2):
        del_copy(r, 0, down).start()
        del_copy(r, 1, down).start()

        @pl.when(can_go[r])
        def _():
            grad_copy(r, 1, z).start()
    for i in range(2):
        for r in range(2):
            dec_copy(r, i, down).start()

            @pl.when(can_go[r])
            def _():
                enc_copy(r, i + 1, z).start()
    for i in range(2, 4):
        for r in range(2):
            dec_copy(r, i, down).start()
    pair_grad(z, core).start()
    for h in range(2):
        pair_copy(z, h, core).start()

    part = rows // 2

    def product_unit(u, low, high):
        q, m, n = u // 4, u // 2 % 2, u % 2
        gap = jnp.maximum(q - z, z - q)
        enc_hop = jnp.where(gap == 0, 0, 2 * gap - 1 + n)
        dec_hop = jnp.where(q == diag, 5 + m, 4)
        hop = jnp.maximum(enc_hop, dec_hop)

        @pl.when(jnp.logical_and(hop >= low, hop <= high))
        def _():
            rs = pl.ds(pl.multiple_of(m * part, part), part)
            acc[n, rs] += jnp.dot(
                dec_all[q, rs, :], enc_all[n, pl.ds(pl.multiple_of(q * depth, 128), depth), :],
                preferred_element_type=F32)

    def products(low, high):
        pl.loop(0, 4 * levels)(lambda u: product_unit(u, low, high))

    def pair_wait(low, high):
        for lv in range(levels):
            for h in range(2):
                gap = jnp.maximum(lv - z, z - lv)
                hop = jnp.where(gap == 0, 0, 2 * gap - 1 + h)

                @pl.when(jnp.logical_and(hop >= low, hop <= high))
                def _():
                    pair_copy(lv, h, 1 - core).wait_recv()

    acc[...] = jnp.zeros_like(acc)

    for k in range(1, 2 * (levels - 1) + 1):
        j, h = (k + 1) // 2, (k - 1) % 2
        for r in range(2):
            if k == 1:
                del_copy(r, 0, ring_from[r]).wait_recv()
                del_copy(r, 2, ring_from[r]).start()
            if k <= 2:
                dec_copy(r, k - 1, ring_from[r]).wait_recv()
                dec_copy(r, k + 3, ring_from[r]).start()
        for r in range(2):
            level = z - step_of[r] * j

            @pl.when(inside(level))
            def _():
                if h == 0:
                    grad_copy(r, j, level).wait_recv()
                    if j < levels - 1:
                        @pl.when(can_go[r])
                        def _():
                            grad_copy(r, j + 1, level).start()
                    pair_grad(level, core).start()
                enc_copy(r, k, level).wait_recv()
                if j < levels - 1:
                    @pl.when(can_go[r])
                    def _():
                        enc_copy(r, k + 2, level).start()
                pair_copy(level, h, core).start()
        if k == 2 * (levels - 2):
            for r in range(2):
                for i in range(2, 4):
                    dec_copy(r, i, ring_from[r]).wait_recv()
            pair_wait(0, 4)
            products(0, 4)
        if k == 2 * (levels - 2) + 1:
            for r in range(2):
                del_copy(r, 1, ring_from[r]).wait_recv()
                del_copy(r, 2, diag).wait_recv()
            for lv in range(levels):
                pair_grad(lv, 1 - core).wait_recv()
            for d in range(n_down):
                for w in range(wins):
                    for b in range(rows // BLOCK):
                        value = jnp.zeros((win, BLOCK), masked.dtype)
                        for s in range(uact):
                            on = flag(upb[s, d * wins + w], b, masked.dtype)
                            value = value + del_all[d, w, :, s * BLOCK:(s + 1) * BLOCK] * on
                        t = (d * wins + w) * win
                        masked[t:t + win, b * BLOCK:(b + 1) * BLOCK] = value
            prod[...] = lax.dot_general(
                masked[...], grad_all[...], (((0,), (0,)), ((), ())), preferred_element_type=F32)

            for r in range(2):
                dec_copy(r, 4, diag).wait_recv()
            pair_wait(5, 5)
            products(5, 5)

    for r in range(2):
        dec_copy(r, 5, diag).wait_recv()
    pair_wait(6, 6)
    products(6, 6)
    stores = []
    for s in range(dact):
        side, at = divmod(s * BLOCK, half)
        res[s] = acc[side, :, at:at + BLOCK] * prod[:, s * BLOCK:(s + 1) * BLOCK]
        stores.append(pltpu.make_async_copy(res.at[s], out.at[s], out_sem.at[s]))
        stores[-1].start()

    for r in range(2):
        for i in range(3):
            del_copy(r, i, down).wait_send()
        for i in range(6):
            dec_copy(r, i, down).wait_send()
        for k in range(1, 2 * (levels - 1) + 1):
            @pl.when(jnp.logical_and(can_go[r], inside(z - step_of[r] * ((k - 1) // 2))))
            def _():
                enc_copy(r, k, z).wait_send()
                if k % 2:
                    grad_copy(r, (k + 1) // 2, z).wait_send()
    for lv in range(levels):
        pair_grad(lv, core).wait_send()
        for h in range(2):
            pair_copy(lv, h, core).wait_send()
    for copy in stores:
        copy.wait()


def spread(downb, scored, out, blank, held, load_sem, out_sem, blank_sem):
    loads = [pltpu.make_async_copy(scored.at[s], held.at[s], load_sem.at[s]) for s in range(downb.shape[0])]
    for copy in loads:
        copy.start()
    blank[...] = jnp.zeros_like(blank)
    blocks = out.shape[1] // BLOCK

    def each_blank(act):
        for c in range(blocks):
            used = sum((downb[s] == c).astype(jnp.int32) for s in range(downb.shape[0]))

            @pl.when(used == 0)
            def _():
                act(pltpu.make_async_copy(blank, out.at[:, c * BLOCK:(c + 1) * BLOCK], blank_sem.at[c]))

    each_blank(lambda copy: copy.start())
    stores = []
    for s, copy in enumerate(loads):
        copy.wait()
        cols = pl.ds(pl.multiple_of(downb[s] * BLOCK, BLOCK), BLOCK)
        stores.append(pltpu.make_async_copy(held.at[s], out.at[:, cols], out_sem.at[s]))
        stores[-1].start()
    each_blank(lambda copy: copy.wait())
    for copy in stores:
        copy.wait()


def ring_local(n_up, n_down, win, deltas, gradients, up_blocks, down_blocks, decoder, encoder):
    rows, depth = decoder.shape
    height, cols = encoder.shape
    toks = gradients.shape[0]
    uact, dact = up_blocks.shape[1], down_blocks.shape[0]
    tokens = deltas.shape[0] * n_down
    wins = deltas.shape[0] // win
    used = dact * BLOCK
    levels = n_up // 2
    kind = decoder.dtype
    dma = pltpu.SemaphoreType.DMA
    smem, anywhere = pl.BlockSpec(memory_space=pltpu.SMEM), pl.BlockSpec(memory_space=pl.ANY)
    hbm = pl.BlockSpec(memory_space=pltpu.HBM)
    hops = 2 * (levels - 1)
    scored = pl.pallas_call(
        functools.partial(gather_scores, n_up, n_down),
        out_shape=jax.ShapeDtypeStruct((dact, rows, BLOCK), F32),
        in_specs=[smem, smem, hbm, hbm, hbm, hbm],
        out_specs=anywhere,
        scratch_shapes=[
            pltpu.VMEM((n_down, rows, depth), kind),
            pltpu.VMEM((height, cols), kind),
            pltpu.VMEM((2, n_up * height, used // 2), kind),
            pltpu.VMEM(deltas.shape, kind),
            pltpu.VMEM((n_down, wins, win, uact * BLOCK), kind),
            pltpu.VMEM((toks, cols), kind),
            pltpu.VMEM((n_up * toks, used), kind),
            pltpu.VMEM((tokens, rows), kind),
            pltpu.VMEM((2, rows, used // 2), F32),
            pltpu.VMEM((rows, used), F32),
            pltpu.VMEM((dact, rows, BLOCK), F32),
            dma((4,)),
            dma((2, 6)), dma((2, 6)),
            dma((2, 3)), dma((2, 3)),
            dma((2, hops)), dma((2, hops)),
            dma((2, levels - 1)), dma((2, levels - 1)),
            dma((levels, 2)), dma((levels, 2)),
            dma((levels,)), dma((levels,)),
            dma((dact,)),
        ],
        compiler_params=pltpu.CompilerParams(collective_id=0, has_side_effects=True, vmem_limit_bytes=LARGE),
        name="gather_scores",
    )(up_blocks.T, down_blocks, deltas, gradients, decoder, encoder)
    return pl.pallas_call(
        spread,
        out_shape=jax.ShapeDtypeStruct((rows, cols), F32),
        in_specs=[smem, anywhere],
        out_specs=anywhere,
        scratch_shapes=[
            pltpu.VMEM((rows, BLOCK), F32),
            pltpu.VMEM((dact, rows, BLOCK), F32),
            dma((dact,)), dma((dact,)), dma((cols // BLOCK,)),
        ],
        compiler_params=pltpu.CompilerParams(vmem_limit_bytes=SMALL),
        name="spread",
    )(down_blocks, scored)


def plain_local(deltas, gradients, up_blocks, down_blocks, decoder, encoder):
    token_deltas = lax.all_gather(deltas, "down", axis=0, tiled=True)
    token_grads = lax.all_gather(gradients, "up", axis=0, tiled=True)
    tokens, rows = token_deltas.shape
    windows, dact = up_blocks.shape[0], down_blocks.shape[0]
    row_blocks, col_blocks = rows // BLOCK, encoder.shape[1] // BLOCK
    local_ids = jnp.arange(row_blocks, dtype=jnp.int32)
    block_on = jnp.any(up_blocks[:, :, None] == local_ids[None, None, :], axis=1)
    masked = token_deltas.reshape(windows, tokens // windows, row_blocks, BLOCK) * block_on[
        :, None, :, None].astype(token_deltas.dtype)
    masked = masked.reshape(tokens, rows)
    dec_whole = lax.all_gather(decoder, "down", axis=1, tiled=True)
    height = encoder.shape[0]
    enc_used = jnp.take(encoder.reshape(height, col_blocks, BLOCK), down_blocks, axis=1).reshape(height, dact * BLOCK)
    virtual = jnp.dot(dec_whole, lax.all_gather(enc_used, "up", axis=0, tiled=True), preferred_element_type=F32)
    grad_used = jnp.take(token_grads.reshape(tokens, col_blocks, BLOCK), down_blocks, axis=1).reshape(tokens, dact * BLOCK)
    product = lax.dot_general(masked, grad_used, (((0,), (0,)), ((), ())), preferred_element_type=F32)
    scored = (product * virtual).reshape(rows, dact, BLOCK)
    filled = jnp.zeros((rows, col_blocks, BLOCK), F32).at[:, down_blocks, :].set(scored)
    return filled.reshape(rows, encoder.shape[1])


def solution(mesh):
    n_up, n_down = mesh.shape["up"], mesh.shape["down"]
    ringed = n_down == 4 and n_up == 2 * n_down

    def local(deltas, gradients, up_blocks, down_blocks, decoder, encoder):
        args = (deltas, gradients, up_blocks, down_blocks, decoder, encoder)
        tokens = deltas.shape[0] * n_down
        win = tokens // up_blocks.shape[0]
        if ringed and deltas.shape[0] == 2 * win:
            return ring_local(n_up, n_down, win, *args)
        return plain_local(*args)

    placed = (P("down", "up"), P("up", "down"), P(None, "up"), P("down"), P("up", "down"), P("up", "down"))
    return jax.shard_map(local, mesh=mesh, in_specs=placed, out_specs=P("up", "down"), check_vma=False)
```

```python
import functools

import jax
import jax.numpy as jnp
from jax import lax
from jax.experimental import pallas as pl
from jax.experimental.pallas import tpu as pltpu
from jax.sharding import PartitionSpec as P

BLOCK = 128
LARGE, SMALL = 24 << 20, 4 << 20
MESH = pl.DeviceIdType.MESH
F32 = jnp.float32


def flag(number, block, kind):
    return jnp.where(jnp.full((1, BLOCK), number, jnp.int32) == block, 1.0, 0.0).astype(kind)


def pick(ref, rows, number, blocks):
    total = None
    for b in range(blocks):
        term = ref[rows, b * BLOCK:(b + 1) * BLOCK] * flag(number, b, ref.dtype)
        total = term if total is None else total + term
    return total


def gather_scores(
    n_up, n_down, upb, downb, deltas, grads, dec, enc, out,
    dec_all, enc_raw, enc_all, del_raw, del_all, grad_raw, grad_all, masked, acc, prod, res,
    load_sem, dec_send, dec_recv, del_send, del_recv, enc_send, enc_recv,
    grad_send, grad_recv, pair_send, pair_recv, pg_send, pg_recv, out_sem,
):
    levels = n_up // 2
    rows, depth = dec.shape
    height = enc.shape[0]
    half = enc_all.shape[2]
    chunk = rows // 4
    toks = grads.shape[0]
    wins = del_all.shape[1]
    win = del_all.shape[2]
    uact = upb.shape[0]
    dact = downb.shape[0]
    up, down = lax.axis_index("up"), lax.axis_index("down")
    z, core = up // 2, up % 2
    place = lambda d: 2 * (d // 2) + (d + d // 2) % 2
    pos = place(down)
    right, left = place((pos + 1) % 4), place((pos + 3) % 4)
    diag = place((pos + 2) % 4)
    ring_to = ((up, right), (up, left))
    ring_from = (left, right)
    step_of = (1, -1)

    loads = [
        pltpu.make_async_copy(dec, dec_all.at[down], load_sem.at[0]),
        pltpu.make_async_copy(enc, enc_raw, load_sem.at[1]),
        pltpu.make_async_copy(deltas, del_raw, load_sem.at[2]),
        pltpu.make_async_copy(grads, grad_raw, load_sem.at[3]),
    ]
    for copy in loads:
        copy.start()

    barrier = pltpu.get_barrier_semaphore()
    can_go = (z < levels - 1, z > 0)
    for dev in (*ring_to, (2 * z + 1 - core, down)):
        pl.semaphore_signal(barrier, inc=1, device_id=dev, device_id_type=MESH)
    for r in range(2):
        @pl.when(can_go[r])
        def _():
            pl.semaphore_signal(barrier, inc=1, device_id=(up + 2 * step_of[r], down), device_id_type=MESH)

    loads[2].wait()
    for w in range(wins):
        for s in range(uact):
            del_all[down, w, :, s * BLOCK:(s + 1) * BLOCK] = pick(
                del_raw, slice(w * win, (w + 1) * win), upb[s, down * wins + w], rows // BLOCK)
    loads[3].wait()
    loads[1].wait()
    for s in range(dact):
        grad_all[pl.ds(pl.multiple_of(up * toks, toks), toks), s * BLOCK:(s + 1) * BLOCK] = pick(
            grad_raw, slice(0, toks), downb[s], enc.shape[1] // BLOCK)
        side, at = divmod(s * BLOCK, half)
        enc_all[side, pl.ds(pl.multiple_of(up * height, 16), height), at:at + BLOCK] = pick(
            enc_raw, slice(0, height), downb[s], enc.shape[1] // BLOCK)
    loads[0].wait()
    expected = 3 + jnp.where(z < levels - 1, 1, 0) + jnp.where(z > 0, 1, 0)
    pl.semaphore_wait(barrier, expected)

    orders = ((0, 2, 1, 3), (1, 3, 0, 2))

    def dec_copy(r, i, owner):
        piece = orders[r][i % 4]
        ref = dec_all.at[owner, pl.ds(piece * chunk, chunk)]
        return pltpu.make_async_remote_copy(
            ref, ref, dec_send.at[r, i], dec_recv.at[r, i], device_id=ring_to[r], device_id_type=MESH)

    def del_copy(r, i, owner):
        piece = (i + r) % 2
        ref = del_all.at[owner, piece]
        return pltpu.make_async_remote_copy(
            ref, ref, del_send.at[r, i], del_recv.at[r, i], device_id=ring_to[r], device_id_type=MESH)

    def enc_rows(level, h, c):
        return enc_all.at[h, pl.ds(pl.multiple_of((level * 2 + c) * height, 16), height)]

    def enc_copy(r, k, level):
        ref = enc_rows(level, (k - 1) % 2, core)
        return pltpu.make_async_remote_copy(
            ref, ref, enc_send.at[r, k - 1], enc_recv.at[r, k - 1],
            device_id=(up + 2 * step_of[r], down), device_id_type=MESH)

    def grad_rows(level, c):
        return grad_all.at[pl.ds(pl.multiple_of((level * 2 + c) * toks, toks), toks)]

    def grad_copy(r, j, level):
        ref = grad_rows(level, core)
        return pltpu.make_async_remote_copy(
            ref, ref, grad_send.at[r, j - 1], grad_recv.at[r, j - 1],
            device_id=(up + 2 * step_of[r], down), device_id_type=MESH)

    def pair_copy(level, h, c):
        ref = enc_rows(level, h, c)
        return pltpu.make_async_remote_copy(
            ref, ref, pair_send.at[level, h], pair_recv.at[level, h],
            device_id=(2 * z + 1 - core, down), device_id_type=MESH)

    def pair_grad(level, c):
        ref = grad_rows(level, c)
        return pltpu.make_async_remote_copy(
            ref, ref, pg_send.at[level], pg_recv.at[level],
            device_id=(2 * z + 1 - core, down), device_id_type=MESH)

    inside = lambda level: jnp.logical_and(level >= 0, level < levels)

    for r in range(2):
        del_copy(r, 0, down).start()
        del_copy(r, 1, down).start()

        @pl.when(can_go[r])
        def _():
            grad_copy(r, 1, z).start()
    for i in range(2):
        for r in range(2):
            dec_copy(r, i, down).start()

            @pl.when(can_go[r])
            def _():
                enc_copy(r, i + 1, z).start()
    for i in range(2, 4):
        for r in range(2):
            dec_copy(r, i, down).start()
    pair_grad(z, core).start()
    for h in range(2):
        pair_copy(z, h, core).start()

    part = rows // 2

    def product_unit(u, low, high):
        q, m, n = u // 4, u // 2 % 2, u % 2
        gap = jnp.maximum(q - z, z - q)
        enc_hop = jnp.where(gap == 0, 0, 2 * gap - 1 + n)
        dec_hop = jnp.where(q == diag, 5 + m, 4)
        hop = jnp.maximum(enc_hop, dec_hop)

        @pl.when(jnp.logical_and(hop >= low, hop <= high))
        def _():
            rs = pl.ds(pl.multiple_of(m * part, part), part)
            acc[n, rs] += jnp.dot(
                dec_all[q, rs, :], enc_all[n, pl.ds(pl.multiple_of(q * depth, 128), depth), :],
                preferred_element_type=F32)

    def products(low, high):
        pl.loop(0, 4 * levels)(lambda u: product_unit(u, low, high))

    def pair_wait(low, high):
        for lv in range(levels):
            for h in range(2):
                gap = jnp.maximum(lv - z, z - lv)
                hop = jnp.where(gap == 0, 0, 2 * gap - 1 + h)

                @pl.when(jnp.logical_and(hop >= low, hop <= high))
                def _():
                    pair_copy(lv, h, 1 - core).wait_recv()

    acc[...] = jnp.zeros_like(acc)

    for k in range(1, 2 * (levels - 1) + 1):
        j, h = (k + 1) // 2, (k - 1) % 2
        for r in range(2):
            if k == 1:
                del_copy(r, 0, ring_from[r]).wait_recv()
                del_copy(r, 2, ring_from[r]).start()
            if k <= 2:
                dec_copy(r, k - 1, ring_from[r]).wait_recv()
                dec_copy(r, k + 3, ring_from[r]).start()
        for r in range(2):
            level = z - step_of[r] * j

            @pl.when(inside(level))
            def _():
                if h == 0:
                    grad_copy(r, j, level).wait_recv()
                    if j < levels - 1:
                        @pl.when(can_go[r])
                        def _():
                            grad_copy(r, j + 1, level).start()
                    pair_grad(level, core).start()
                enc_copy(r, k, level).wait_recv()
                if j < levels - 1:
                    @pl.when(can_go[r])
                    def _():
                        enc_copy(r, k + 2, level).start()
                pair_copy(level, h, core).start()
        if k == 2 * (levels - 2):
            for r in range(2):
                for i in range(2, 4):
                    dec_copy(r, i, ring_from[r]).wait_recv()
            pair_wait(0, 4)
            products(0, 4)
        if k == 2 * (levels - 2) + 1:
            for r in range(2):
                del_copy(r, 1, ring_from[r]).wait_recv()
                del_copy(r, 2, diag).wait_recv()
            for lv in range(levels):
                pair_grad(lv, 1 - core).wait_recv()
            for d in range(n_down):
                for w in range(wins):
                    for b in range(rows // BLOCK):
                        value = jnp.zeros((win, BLOCK), masked.dtype)
                        for s in range(uact):
                            on = flag(upb[s, d * wins + w], b, masked.dtype)
                            value = value + del_all[d, w, :, s * BLOCK:(s + 1) * BLOCK] * on
                        t = (d * wins + w) * win
                        masked[t:t + win, b * BLOCK:(b + 1) * BLOCK] = value
            prod[...] = lax.dot_general(
                masked[...], grad_all[...], (((0,), (0,)), ((), ())), preferred_element_type=F32)

            for r in range(2):
                dec_copy(r, 4, diag).wait_recv()
            pair_wait(5, 5)
            products(5, 5)

    for r in range(2):
        dec_copy(r, 5, diag).wait_recv()
    pair_wait(6, 6)
    products(6, 6)
    stores = []
    for s in range(dact):
        side, at = divmod(s * BLOCK, half)
        res[s] = acc[side, :, at:at + BLOCK] * prod[:, s * BLOCK:(s + 1) * BLOCK]
        stores.append(pltpu.make_async_copy(res.at[s], out.at[s], out_sem.at[s]))
        stores[-1].start()

    for r in range(2):
        for i in range(3):
            del_copy(r, i, down).wait_send()
        for i in range(6):
            dec_copy(r, i, down).wait_send()
        for k in range(1, 2 * (levels - 1) + 1):
            @pl.when(jnp.logical_and(can_go[r], inside(z - step_of[r] * ((k - 1) // 2))))
            def _():
                enc_copy(r, k, z).wait_send()
                if k % 2:
                    grad_copy(r, (k + 1) // 2, z).wait_send()
    for lv in range(levels):
        pair_grad(lv, core).wait_send()
        for h in range(2):
            pair_copy(lv, h, core).wait_send()
    for copy in stores:
        copy.wait()


def spread(downb, scored, out, blank, held, load_sem, out_sem, blank_sem):
    loads = [pltpu.make_async_copy(scored.at[s], held.at[s], load_sem.at[s]) for s in range(downb.shape[0])]
    for copy in loads:
        copy.start()
    blank[...] = jnp.zeros_like(blank)
    blocks = out.shape[1] // BLOCK

    def each_blank(act):
        for c in range(blocks):
            used = sum((downb[s] == c).astype(jnp.int32) for s in range(downb.shape[0]))

            @pl.when(used == 0)
            def _():
                act(pltpu.make_async_copy(blank, out.at[:, c * BLOCK:(c + 1) * BLOCK], blank_sem.at[c]))

    each_blank(lambda copy: copy.start())
    stores = []
    for s, copy in enumerate(loads):
        copy.wait()
        cols = pl.ds(pl.multiple_of(downb[s] * BLOCK, BLOCK), BLOCK)
        stores.append(pltpu.make_async_copy(held.at[s], out.at[:, cols], out_sem.at[s]))
        stores[-1].start()
    each_blank(lambda copy: copy.wait())
    for copy in stores:
        copy.wait()


def ring_local(n_up, n_down, win, deltas, gradients, up_blocks, down_blocks, decoder, encoder):
    rows, depth = decoder.shape
    height, cols = encoder.shape
    toks = gradients.shape[0]
    uact, dact = up_blocks.shape[1], down_blocks.shape[0]
    tokens = deltas.shape[0] * n_down
    wins = deltas.shape[0] // win
    used = dact * BLOCK
    levels = n_up // 2
    kind = decoder.dtype
    dma = pltpu.SemaphoreType.DMA
    smem, anywhere = pl.BlockSpec(memory_space=pltpu.SMEM), pl.BlockSpec(memory_space=pl.ANY)
    hbm = pl.BlockSpec(memory_space=pltpu.HBM)
    hops = 2 * (levels - 1)
    scored = pl.pallas_call(
        functools.partial(gather_scores, n_up, n_down),
        out_shape=jax.ShapeDtypeStruct((dact, rows, BLOCK), F32),
        in_specs=[smem, smem, hbm, hbm, hbm, hbm],
        out_specs=anywhere,
        scratch_shapes=[
            pltpu.VMEM((n_down, rows, depth), kind),
            pltpu.VMEM((height, cols), kind),
            pltpu.VMEM((2, n_up * height, used // 2), kind),
            pltpu.VMEM(deltas.shape, kind),
            pltpu.VMEM((n_down, wins, win, uact * BLOCK), kind),
            pltpu.VMEM((toks, cols), kind),
            pltpu.VMEM((n_up * toks, used), kind),
            pltpu.VMEM((tokens, rows), kind),
            pltpu.VMEM((2, rows, used // 2), F32),
            pltpu.VMEM((rows, used), F32),
            pltpu.VMEM((dact, rows, BLOCK), F32),
            dma((4,)),
            dma((2, 6)), dma((2, 6)),
            dma((2, 3)), dma((2, 3)),
            dma((2, hops)), dma((2, hops)),
            dma((2, levels - 1)), dma((2, levels - 1)),
            dma((levels, 2)), dma((levels, 2)),
            dma((levels,)), dma((levels,)),
            dma((dact,)),
        ],
        compiler_params=pltpu.CompilerParams(collective_id=0, has_side_effects=True, vmem_limit_bytes=LARGE),
        name="gather_scores",
    )(*[pltpu.with_memory_space_constraint(x, pltpu.HBM) for x in (up_blocks.T, down_blocks, deltas, gradients, decoder, encoder)])
    return pl.pallas_call(
        spread,
        out_shape=jax.ShapeDtypeStruct((rows, cols), F32),
        in_specs=[smem, anywhere],
        out_specs=anywhere,
        scratch_shapes=[
            pltpu.VMEM((rows, BLOCK), F32),
            pltpu.VMEM((dact, rows, BLOCK), F32),
            dma((dact,)), dma((dact,)), dma((cols // BLOCK,)),
        ],
        compiler_params=pltpu.CompilerParams(vmem_limit_bytes=SMALL),
        name="spread",
    )(pltpu.with_memory_space_constraint(down_blocks, pltpu.HBM), scored)


def plain_local(deltas, gradients, up_blocks, down_blocks, decoder, encoder):
    token_deltas = lax.all_gather(deltas, "down", axis=0, tiled=True)
    token_grads = lax.all_gather(gradients, "up", axis=0, tiled=True)
    tokens, rows = token_deltas.shape
    windows, dact = up_blocks.shape[0], down_blocks.shape[0]
    row_blocks, col_blocks = rows // BLOCK, encoder.shape[1] // BLOCK
    local_ids = jnp.arange(row_blocks, dtype=jnp.int32)
    block_on = jnp.any(up_blocks[:, :, None] == local_ids[None, None, :], axis=1)
    masked = token_deltas.reshape(windows, tokens // windows, row_blocks, BLOCK) * block_on[
        :, None, :, None].astype(token_deltas.dtype)
    masked = masked.reshape(tokens, rows)
    dec_whole = lax.all_gather(decoder, "down", axis=1, tiled=True)
    height = encoder.shape[0]
    enc_used = jnp.take(encoder.reshape(height, col_blocks, BLOCK), down_blocks, axis=1).reshape(height, dact * BLOCK)
    virtual = jnp.dot(dec_whole, lax.all_gather(enc_used, "up", axis=0, tiled=True), preferred_element_type=F32)
    grad_used = jnp.take(token_grads.reshape(tokens, col_blocks, BLOCK), down_blocks, axis=1).reshape(tokens, dact * BLOCK)
    product = lax.dot_general(masked, grad_used, (((0,), (0,)), ((), ())), preferred_element_type=F32)
    scored = (product * virtual).reshape(rows, dact, BLOCK)
    filled = jnp.zeros((rows, col_blocks, BLOCK), F32).at[:, down_blocks, :].set(scored)
    return filled.reshape(rows, encoder.shape[1])


def solution(mesh):
    n_up, n_down = mesh.shape["up"], mesh.shape["down"]
    ringed = n_down == 4 and n_up == 2 * n_down

    def local(deltas, gradients, up_blocks, down_blocks, decoder, encoder):
        args = (deltas, gradients, up_blocks, down_blocks, decoder, encoder)
        tokens = deltas.shape[0] * n_down
        win = tokens // up_blocks.shape[0]
        if ringed and deltas.shape[0] == 2 * win:
            return ring_local(n_up, n_down, win, *args)
        return plain_local(*args)

    placed = (P("down", "up"), P("up", "down"), P(None, "up"), P("down"), P("up", "down"), P("up", "down"))
    return jax.shard_map(local, mesh=mesh, in_specs=placed, out_specs=P("up", "down"), check_vma=False)
```
